32 devices in a mesh: rep: 2 (over x), span: 2 (over core), seq: 8 (over z, y).
Axes of the slice: x: 2, y: 2, z: 4, core: 2. Of those that a mesh axis runs over, the one named last changes fastest.
Arguments:
- queries: bfloat16 [4096, 2, 4096], P(('rep', 'span', 'seq')), parts along dimension 0, may hold values from -40 to 40
- keys: bfloat16 [4096, 2, 4096], P(('rep', 'span', 'seq')), parts along dimension 0, may hold values from -16 to 16
- values: bfloat16 [4096, 2, 4096], P(('rep', 'span', 'seq')), parts along dimension 0, may hold values from -6 to 6
- cache_keys: bfloat16 [1024, 2, 4096], P(('rep', 'span'), None, 'seq'), parts along dimension 0, may hold values from -9 to 9
- cache_values: bfloat16 [1024, 2, 4096], P(('rep', 'span'), None, 'seq'), parts along dimension 0, may hold values from -6 to 6
- span_lengths: int32 [4], P('rep'), parts along dimension 0, may hold values from 512 to 1024, as said below
- cache_offsets: int32 [4], P('rep'), parts along dimension 0, may hold values from 0 to 256
- step_index: int32 [4], P('rep'), parts along dimension 0, may hold values from 0 to 63
- step_gain: float32 [64, 4096], replicated, may hold values from -12 to 12
Outputs:
- attended: bfloat16 [4096, 2, 4096], P(('rep', 'span', 'seq')), parts along dimension 0
The draws below stay inside these ranges and needn't reach their ends.
There are 2 independent parts, one for each index of `rep`. The reference program is written for one: setup_inputs(seed, part) draws one part's arguments, and reference() takes and returns one part's arrays. A program takes and returns all parts, laid end to end along the dimension named above; an argument that names none is the same for every part. Nothing has to cross between parts.
Inputs may be any that keep to these rules, and one draw needn't show every extreme that they name: `span_lengths`: at least one span has all 1024 tokens live; every span has at least 512.
All inputs are finite; a program needn't handle non-finite values.
Results may differ from the reference program's by a relative error of at most 0.015.
Values may be sent and summed in bfloat16 or wider, within the bound.
A program may use at most 128 MiB of HBM per device.

```python
import jax
import jax.numpy as jnp
from jax import lax

D = 4096
HEADS = 32
HD = 128
STEPS = 64
SPAN_LEN = 1024
WINDOW = 2048
CACHE_TOK = 512
N_SPAN = 2


def draw_keys(key, part):
    drawn = 1.5 * jnp.clip(jax.random.normal(jax.random.fold_in(key, 1), (WINDOW, 2, D), jnp.float32), -6.0, 6.0)
    return drawn.astype(jnp.bfloat16)


def draw_queries(key, part):
    drawn = 1.5 * jnp.clip(jax.random.normal(jax.random.fold_in(key, 2), (WINDOW, 2, D), jnp.float32), -6.0, 6.0)
    return drawn.astype(jnp.bfloat16)


def draw_span_lengths(key, part):
    drawn = jax.random.randint(jax.random.fold_in(key, 3), (N_SPAN,), SPAN_LEN // 2, SPAN_LEN + 1)
    full_section = jax.random.randint(jax.random.fold_in(key, 4), (), 0, N_SPAN)
    return jnp.where(jnp.arange(N_SPAN) == full_section, SPAN_LEN, drawn).astype(jnp.int32)


def block_levels(key, extent, pieces, least, top_value):
    loudness, own = 1.0, jax.random.fold_in(key, 6)
    for position, blocks in pieces:
        steps = jnp.exp(jax.random.uniform(jax.random.fold_in(own, position), (blocks,), jnp.float32, least / len(pieces), top_value / len(pieces)))
        loudness = loudness * jnp.repeat(steps, extent[position] // blocks).reshape([-1 if axis == position else 1 for axis in range(len(extent))])
    return loudness


def centred(stream_key, dims, deviation, most, pieces=(), held_as=jnp.bfloat16):
    result = jax.random.normal(stream_key, dims, jnp.float32) * deviation
    if len(pieces) > 0:
        result = block_levels(stream_key, dims, pieces, -0.22, 0.18) * result
    return jnp.clip(result, min=-most, max=most).astype(held_as)


def setup_inputs(seed: int = 0, part: int = 0) -> dict:
    key_list = jax.random.split(jax.random.key(seed), 10)
    own_keys = jax.random.split(jax.random.fold_in(key_list[9], part), 10)
    return {
        "queries": draw_queries(jax.random.fold_in(jax.random.fold_in(key_list[9], part), 71), part),
        "keys": draw_keys(jax.random.fold_in(jax.random.fold_in(key_list[9], part), 71), part),
        "values": centred(own_keys[2], (WINDOW, 2, D), 1.0, 6.0, ((0, 16),)),
        "cache_keys": centred(own_keys[3], (CACHE_TOK, 2, D), 1.5, 9.0, ((0, 2), (2, 8))),
        "cache_values": centred(own_keys[4], (CACHE_TOK, 2, D), 1.0, 6.0, ((0, 2), (2, 8))),
        "span_lengths": draw_span_lengths(jax.random.fold_in(jax.random.fold_in(key_list[9], part), 71), part),
        "cache_offsets": jax.random.randint(own_keys[6], (N_SPAN,), 0, CACHE_TOK // 2 + 1).astype(jnp.int32),
        "step_index": jax.random.randint(own_keys[7], (N_SPAN,), 0, STEPS).astype(jnp.int32),
        "step_gain": centred(key_list[8], (STEPS, D), 3.0, 12.0, (), jnp.float32),
    }


masked_score = -1e30


def by_heads(tensor):
    return tensor.reshape(tensor.shape[0], 2 * HEADS, HD).transpose(1, 0, 2)


def reference(queries, keys, values, cache_keys, cache_values, span_lengths, cache_offsets, step_index, step_gain):
    positions = jnp.arange(SPAN_LEN, dtype=jnp.int32)
    cache_positions = jnp.arange(CACHE_TOK, dtype=jnp.int32)
    results = []
    for section in range(N_SPAN):
        first_row = section * SPAN_LEN
        query_block = queries[first_row:first_row + SPAN_LEN]
        key_block = jnp.concatenate([cache_keys, keys[:first_row + SPAN_LEN]], 0)
        value_block = jnp.concatenate([cache_values, values[:first_row + SPAN_LEN]], 0)
        visible = jnp.concatenate([cache_positions >= cache_offsets[section]] + [positions < span_lengths[earlier] for earlier in range(section + 1)], 0)

        def attend(operands):
            query_head, key_head, value_head = operands
            scores = jnp.dot(query_head, key_head.T, preferred_element_type=jnp.float32) * (HD ** -0.5)
            scores = jnp.where(visible[None, :], scores, masked_score)
            largest = jnp.max(scores, axis=1, keepdims=True)
            weights = jnp.where(visible[None, :], jnp.exp(scores - largest), 0.0)
            total = jnp.sum(weights, axis=1, keepdims=True)
            return jnp.dot(weights.astype(jnp.bfloat16), value_head, preferred_element_type=jnp.float32) / total

        output = lax.map(attend, (by_heads(query_block), by_heads(key_block), by_heads(value_block)))
        output = output.transpose(1, 0, 2).reshape(SPAN_LEN, 2, D)
        row_gain = step_gain[step_index[section]]
        results.append((output * row_gain).astype(jnp.bfloat16))
    return jnp.concatenate(results, 0)
```

```python
import functools

import jax
import jax.numpy as jnp
from jax import lax
from jax.experimental import pallas as pl
from jax.experimental.pallas import tpu as pltpu
from jax.sharding import PartitionSpec as P

HD = 128
MESH = pl.DeviceIdType.MESH
masked_score = -1e30
KEYS, VALUES, QUERIES, OUTS = range(4)


def kernel(
    n_seq,
    n_span,
    q_ref,
    k_ref,
    v_ref,
    ck_ref,
    cv_ref,
    length_ref,
    offset_ref,
    step_ref,
    gain_ref,
    out_ref,
    kraw,
    vraw,
    qraw,
    oraw,
    ckraw,
    cvraw,
    kd,
    vd,
    qd,
    od,
    stage,
    bias,
    gain,
    row_gains,
    send_sem,
    recv_sem,
    cache_send,
    cache_recv,
    local_sem,
):
    n = n_seq * n_span
    seq, span = lax.axis_index("seq"), lax.axis_index("span")
    tokens, members, width = kraw.shape[1:]
    heads = width // HD
    piece = ckraw.shape[1]
    cached = n_span * piece
    scale = HD ** (-0.5)
    my_group = seq * n_span + span
    my_slot = span * n_seq + seq

    def ahead(k):
        return (
            lax.rem(seq + lax.div(k, n_span), n_seq),
            lax.rem(span + lax.rem(k, n_span), n_span),
        )

    def behind(k):
        return (
            lax.rem(seq + n_seq - lax.div(k, n_span), n_seq),
            lax.rem(span + n_span - lax.rem(k, n_span), n_span),
        )

    half = n_seq // 4
    run = 2 * n_span
    my_pair = lax.div(seq, 2)
    upper = lax.div(my_pair, half)
    lower = 1 - upper
    depth = my_pair - upper * half
    outer = lower * (1 - lax.div(depth, half - half // 2)) + upper * lax.div(depth, half // 2)

    def near_pair(i):
        return upper * half + lax.rem(depth + i, half)

    def far_pair(i):
        return lower * (2 * half - 1 - i) + upper * i

    def far_target(i):
        inwards = outer * i + (1 - outer) * (half - 1 - i)
        return far_pair(inwards)

    def near_then_far(i, far_order=far_pair):
        far = lax.div(i, half)
        return (1 - far) * near_pair(i) + far * far_order(i - half)

    def far_then_near(i):
        near = lax.div(i, half)
        return near * near_pair(i - half) + (1 - near) * far_target(i)

    def member_of(pair, r):
        return (2 * pair + lax.div(r, n_span), lax.rem(r, n_span))

    def lag_to(place):
        return lax.rem(place[0] - seq + n_seq, n_seq) * n_span + lax.rem(
            place[1] - span + n_span, n_span
        )

    def lag_from(place):
        return lax.rem(seq - place[0] + n_seq, n_seq) * n_span + lax.rem(
            span - place[1] + n_span, n_span
        )

    def columns(group):
        return pl.ds(pl.multiple_of(group * width, HD), width)

    def group_of(place):
        return place[0] * n_span + place[1]

    def slot_of(place):
        return place[1] * n_seq + place[0]

    def device(place):
        return {"seq": place[0], "span": place[1]}

    sources = (k_ref, v_ref, q_ref)
    landings = (kraw, vraw, qraw)

    def scatter(kind, k):
        to = ahead(k)
        return pltpu.make_async_remote_copy(
            src_ref=sources[kind].at[:, :, columns(group_of(to))],
            dst_ref=landings[kind].at[my_slot],
            send_sem=send_sem.at[kind, k],
            recv_sem=recv_sem.at[kind, k],
            device_id=device(to),
            device_id_type=MESH,
        )

    def arrival(kind, k):
        origin = behind(k)
        return pltpu.make_async_remote_copy(
            src_ref=sources[kind].at[:, :, columns(group_of(origin))],
            dst_ref=landings[kind].at[slot_of(origin)],
            send_sem=send_sem.at[kind, k],
            recv_sem=recv_sem.at[kind, k],
            device_id=device(origin),
            device_id_type=MESH,
        )

    def give_back(k):
        to = behind(k)
        return pltpu.make_async_remote_copy(
            src_ref=oraw.at[k],
            dst_ref=out_ref.at[:, :, columns(my_group)],
            send_sem=send_sem.at[OUTS, k],
            recv_sem=recv_sem.at[OUTS, k],
            device_id=device(to),
            device_id_type=MESH,
        )

    def returned(k):
        origin = ahead(k)
        return pltpu.make_async_remote_copy(
            src_ref=oraw.at[k],
            dst_ref=out_ref.at[:, :, columns(group_of(origin))],
            send_sem=send_sem.at[OUTS, k],
            recv_sem=recv_sem.at[OUTS, k],
            device_id=device(origin),
            device_id_type=MESH,
        )

    cache_pairs = ((ck_ref, ckraw), (cv_ref, cvraw))

    def cache_copy(which, b, to_span, from_span):
        source, landing = cache_pairs[which]
        return pltpu.make_async_remote_copy(
            src_ref=source.at[:, :, columns(to_span)],
            dst_ref=landing.at[from_span],
            send_sem=cache_send.at[which, b],
            recv_sem=cache_recv.at[which, b],
            device_id={"span": to_span},
            device_id_type=MESH,
        )

    own_copies = [
        pltpu.make_async_copy(
            sources[kind].at[:, :, columns(my_group)],
            landings[kind].at[my_slot],
            local_sem.at[kind],
        )
        for kind in range(3)
    ] + [
        pltpu.make_async_copy(
            cache_pairs[which][0].at[:, :, columns(span)],
            cache_pairs[which][1].at[span],
            local_sem.at[3 + which],
        )
        for which in range(2)
    ] + [
        pltpu.make_async_copy(gain_ref.at[:, columns(my_group)], gain, local_sem.at[5])
    ]

    barrier = pltpu.get_barrier_semaphore()

    @pl.loop(1, n)
    def _(k):
        pl.semaphore_signal(barrier, inc=1, device_id=device(ahead(k)), device_id_type=MESH)

    for copy in own_copies:
        copy.start()
    pl.semaphore_wait(barrier, n - 1)

    for b in range(1, n_span):
        for which in range(2):
            cache_copy(which, b, lax.rem(span + b, n_span), span).start()

    def scatter_all(kind, order):
        @pl.loop(0, n)
        def _(j):
            shifted = lax.rem(j + lax.rem(my_group, run), run)
            k = lag_to(member_of(order(lax.div(j, run)), shifted))

            @pl.when(k > 0)
            def _():
                scatter(kind, k).start()

    scatter_all(KEYS, far_then_near)
    scatter_all(VALUES, far_then_near)

    @pl.when(outer == 0)
    def _():
        scatter_all(QUERIES, functools.partial(near_then_far, far_order=far_target))

    def separate(block, target, row):
        for h in range(heads):
            stage[h] = (
                block[:, :, h * HD : (h + 1) * HD].reshape(members * tokens, HD).astype(jnp.float32)
            )
            for m in range(members):
                target[h * members + m, pl.ds(row, tokens), :] = stage[
                    h, pl.ds(m, tokens, stride=members), :
                ].astype(jnp.bfloat16)

    span_len = n_seq * tokens
    places = lax.broadcasted_iota(jnp.int32, (1, cached), 1)
    live = lax.broadcasted_iota(jnp.int32, (1, span_len), 1)
    for c in range(n_span):
        bias[c : c + 1, 0:cached] = jnp.where(places >= offset_ref[c], 0.0, masked_score)
        for e in range(c + 1):
            first = cached + e * span_len
            bias[c : c + 1, first : first + span_len] = jnp.where(
                live < length_ref[e], 0.0, masked_score
            )
    for copy in own_copies:
        copy.wait()
    levels = lax.broadcasted_iota(jnp.int32, gain.shape, 0)
    for c in range(n_span):
        row_gains[c : c + 1] = jnp.sum(
            jnp.where(levels == step_ref[c], gain[...], 0.0), axis=0, keepdims=True
        )
    for b in range(1, n_span):
        for which in range(2):
            origin = lax.rem(span + n_span - b, n_span)
            cache_copy(which, b, origin, origin).wait_recv()
    for which, target in ((0, kd), (1, vd)):
        for e in range(n_span):

            @pl.loop(0, piece // tokens)
            def _(i, which=which, target=target, e=e):
                row = pl.multiple_of(i * tokens, tokens)
                block = cache_pairs[which][1].at[e, pl.ds(row, tokens)]
                separate(block, target, pl.multiple_of(e * piece + row, tokens))

    def window_row(slot):
        return pl.multiple_of(cached + slot * tokens, tokens)

    for kind, target in ((KEYS, kd), (VALUES, vd)):
        separate(landings[kind].at[my_slot], target, window_row(my_slot))

        @pl.loop(0, n)
        def _(j, kind=kind, target=target):
            k = lag_from(member_of(near_then_far(lax.div(j, run)), lax.rem(j, run)))

            @pl.when(k > 0)
            def _():
                slot = slot_of(behind(k))
                arrival(kind, k).wait_recv()
                separate(landings[kind].at[slot], target, window_row(slot))

    @pl.when(outer == 1)
    def _():
        scatter_all(QUERIES, functools.partial(near_then_far, far_order=far_target))

    def turn_lags(t):
        pair = near_then_far(lax.div(t, n_span))
        block_span = lax.rem(t, n_span)
        return [lag_from((2 * pair + i, block_span)) for i in range(2)]

    last_pair = n // 2 - n_span

    @pl.loop(0, n // 2)
    def _(t):
        offsets = turn_lags(t)
        block_span = lax.rem(t, n_span)
        for i, k in enumerate(offsets):

            @pl.when(k > 0)
            def _(k=k):
                arrival(QUERIES, k).wait_recv()

            separate(qraw.at[slot_of(behind(k))], qd, i * tokens)

        @pl.when((outer == 1) & (t == last_pair))
        def _():
            @pl.loop(half * n_span, last_pair)
            def _(earlier):
                for k in turn_lags(earlier):
                    give_back(k).start()

        for c in range(n_span):

            @pl.when(block_span == c)
            def _(c=c):
                length = cached + (c + 1) * n_seq * tokens

                @pl.loop(0, heads * members)
                def _(g):
                    scores = lax.dot_general(
                        qd[g],
                        kd[g, pl.ds(0, length), :],
                        (((1,), (1,)), ((), ())),
                        preferred_element_type=jnp.float32,
                    )
                    scores = scores * scale + bias[c : c + 1, pl.ds(0, length)]
                    largest = jnp.max(scores, axis=1, keepdims=True)
                    weights = jnp.exp(scores - largest)
                    total = jnp.sum(weights, axis=1, keepdims=True)
                    od[g] = (
                        jnp.dot(
                            weights.astype(jnp.bfloat16),
                            vd[g, pl.ds(0, length), :],
                            preferred_element_type=jnp.float32,
                        )
                        / total
                    )

                for i, k in enumerate(offsets):
                    for h in range(heads):
                        row_gain = row_gains[c : c + 1, h * HD : (h + 1) * HD]
                        for m in range(members):
                            stage[h, pl.ds(m, tokens, stride=members), :] = (
                                od[h * members + m, i * tokens : (i + 1) * tokens, :] * row_gain
                            )
                        oraw[k, :, :, h * HD : (h + 1) * HD] = (
                            stage[h].astype(jnp.bfloat16).reshape(tokens, members, HD)
                        )

        held_back = (outer == 1) & (t >= half * n_span) & (t < last_pair)
        for k in offsets:

            @pl.when((k > 0) & jnp.logical_not(held_back))
            def _(k=k):
                give_back(k).start()

    last = pltpu.make_async_copy(
        oraw.at[0], out_ref.at[:, :, columns(my_group)], local_sem.at[6]
    )
    last.start()

    @pl.loop(1, n)
    def _(k):
        for kind in range(3):
            scatter(kind, k).wait_send()
        give_back(k).wait_send()
        returned(k).wait_recv()

    for b in range(1, n_span):
        for which in range(2):
            cache_copy(which, b, lax.rem(span + b, n_span), span).wait_send()
    last.wait()


def hand_over(pieces, source, target, held, in_sem, out_sem):
    rows = held.shape[0] // pieces
    parts = [pl.ds(i * rows, rows) for i in range(pieces)]
    inward = [
        pltpu.make_async_copy(source.at[part], held.at[part], in_sem.at[i])
        for i, part in enumerate(parts)
    ]
    outward = [
        pltpu.make_async_copy(held.at[part], target.at[part], out_sem.at[i])
        for i, part in enumerate(parts)
    ]
    for copy in inward:
        copy.start()
    for arriving, leaving in zip(inward, outward):
        arriving.wait()
        leaving.start()
    for copy in outward:
        copy.wait()


def per_device(
    queries,
    keys,
    values,
    cache_keys,
    cache_values,
    span_lengths,
    cache_offsets,
    step_index,
    step_gain,
):
    n_seq, n_span = lax.axis_size("seq"), lax.axis_size("span")
    n = n_seq * n_span
    tokens, members, features = queries.shape
    width = features // n
    groups = members * width // HD
    piece = cache_keys.shape[0]
    cached, span_len = n_span * piece, n_seq * tokens
    full = cached + n_span * span_len

    anywhere = pl.BlockSpec(memory_space=pl.ANY)
    scalars = pl.BlockSpec(memory_space=pltpu.SMEM)
    block = (n, tokens, members, width)
    attended = pl.pallas_call(
        functools.partial(kernel, n_seq, n_span),
        out_shape=jax.ShapeDtypeStruct(queries.shape, jnp.bfloat16),
        in_specs=[anywhere] * 5 + [scalars] * 3 + [anywhere],
        out_specs=anywhere,
        scratch_shapes=[pltpu.VMEM(block, jnp.bfloat16)] * 4
        + [pltpu.VMEM((n_span, piece, members, width), jnp.bfloat16)] * 2
        + [pltpu.VMEM((groups, full, HD), jnp.bfloat16)] * 2
        + [
            pltpu.VMEM((groups, 2 * tokens, HD), jnp.bfloat16),
            pltpu.VMEM((groups, 2 * tokens, HD), jnp.float32),
            pltpu.VMEM((width // HD, members * tokens, HD), jnp.float32),
            pltpu.VMEM((n_span, full), jnp.float32),
            pltpu.VMEM((step_gain.shape[0], width), jnp.float32),
            pltpu.VMEM((n_span, width), jnp.float32),
            pltpu.SemaphoreType.DMA((4, n)),
            pltpu.SemaphoreType.DMA((4, n)),
            pltpu.SemaphoreType.DMA((2, n_span)),
            pltpu.SemaphoreType.DMA((2, n_span)),
            pltpu.SemaphoreType.DMA((7,)),
        ],
        compiler_params=pltpu.CompilerParams(
            collective_id=0, has_side_effects=True, vmem_limit_bytes=60 * 2**20
        ),
    )(
        queries,
        keys,
        values,
        cache_keys,
        cache_values,
        span_lengths,
        cache_offsets,
        step_index,
        step_gain,
    )
    pieces = 8
    return pl.pallas_call(
        functools.partial(hand_over, pieces),
        out_shape=jax.ShapeDtypeStruct(queries.shape, jnp.bfloat16),
        in_specs=[anywhere],
        out_specs=anywhere,
        scratch_shapes=[
            pltpu.VMEM(queries.shape, jnp.bfloat16),
            pltpu.SemaphoreType.DMA((pieces,)),
            pltpu.SemaphoreType.DMA((pieces,)),
        ],
    )(attended)


def solution(mesh):
    placed = (
        P(("rep", "span", "seq"), None, None),
        P(("rep", "span", "seq"), None, None),
        P(("rep", "span", "seq"), None, None),
        P(("rep", "span"), None, "seq"),
        P(("rep", "span"), None, "seq"),
        P("rep"),
        P("rep"),
        P("rep"),
        P(),
    )
    return jax.shard_map(
        per_device,
        mesh=mesh,
        in_specs=placed,
        out_specs=P(("rep", "span", "seq"), None, None),
        check_vma=False,
    )
```

```python
import functools

import jax
import jax.numpy as jnp
from jax import lax
from jax.experimental import pallas as pl
from jax.experimental.pallas import tpu as pltpu
from jax.sharding import PartitionSpec as P

HD = 128
MESH = pl.DeviceIdType.MESH
masked_score = -1e30
KEYS, VALUES, QUERIES, OUTS = range(4)


def kernel(
    n_seq,
    n_span,
    q_ref,
    k_ref,
    v_ref,
    ck_ref,
    cv_ref,
    length_ref,
    offset_ref,
    step_ref,
    gain_ref,
    out_ref,
    kraw,
    vraw,
    qraw,
    oraw,
    ckraw,
    cvraw,
    kd,
    vd,
    qd,
    od,
    stage,
    bias,
    gain,
    row_gains,
    send_sem,
    recv_sem,
    back_sem,
    cache_send,
    cache_recv,
    local_sem,
):
    n = n_seq * n_span
    seq, span = lax.axis_index("seq"), lax.axis_index("span")
    tokens, members, width = kraw.shape[1:]
    heads = width // HD
    piece = ckraw.shape[1]
    cached = n_span * piece
    scale = HD ** (-0.5)
    my_group = seq * n_span + span
    my_slot = span * n_seq + seq

    def ahead(k):
        return (
            lax.rem(seq + lax.div(k, n_span), n_seq),
            lax.rem(span + lax.rem(k, n_span), n_span),
        )

    def behind(k):
        return (
            lax.rem(seq + n_seq - lax.div(k, n_span), n_seq),
            lax.rem(span + n_span - lax.rem(k, n_span), n_span),
        )

    half = n_seq // 4
    run = 2 * n_span
    my_pair = lax.div(seq, 2)
    upper = lax.div(my_pair, half)
    lower = 1 - upper
    depth = my_pair - upper * half
    outer = lower * (1 - lax.div(depth, half - half // 2)) + upper * lax.div(depth, half // 2)

    def near_pair(i):
        return upper * half + lax.rem(depth + i, half)

    def far_pair(i):
        return lower * (2 * half - 1 - i) + upper * i

    def near_then_far(i):
        far = lax.div(i, half)
        return (1 - far) * near_pair(i) + far * far_pair(i - half)

    def member_of(pair, r):
        return (2 * pair + lax.div(r, n_span), lax.rem(r, n_span))

    def lag_from(place):
        return lax.rem(seq - place[0] + n_seq, n_seq) * n_span + lax.rem(
            span - place[1] + n_span, n_span
        )

    def columns(group):
        return pl.ds(pl.multiple_of(group * width, HD), width)

    def group_of(place):
        return place[0] * n_span + place[1]

    def slot_of(place):
        return place[1] * n_seq + place[0]

    def device(place):
        return {"seq": place[0], "span": place[1]}

    sources = (k_ref, v_ref, q_ref)
    landings = (kraw, vraw, qraw)

    def scatter(kind, to):
        return pltpu.make_async_remote_copy(
            src_ref=sources[kind].at[:, :, columns(group_of(to))],
            dst_ref=landings[kind].at[my_slot],
            send_sem=send_sem.at[kind],
            recv_sem=recv_sem.at[kind, my_pair],
            device_id=device(to),
            device_id_type=MESH,
        )

    def take(blocks, sem):
        many = kraw.at[pl.ds(0, blocks)]
        pltpu.make_async_copy(many, many, sem).wait()

    def arrival(kind, i, pair):
        @pl.when(i == 0)
        def _():
            take(run - 1, recv_sem.at[kind, pair])

        @pl.when(i > 0)
        def _():
            take(run, recv_sem.at[kind, pair])

    def give_back(k):
        to = behind(k)
        return pltpu.make_async_remote_copy(
            src_ref=oraw.at[k],
            dst_ref=out_ref.at[:, :, columns(my_group)],
            send_sem=send_sem.at[OUTS],
            recv_sem=back_sem,
            device_id=device(to),
            device_id_type=MESH,
        )

    cache_pairs = ((ck_ref, ckraw), (cv_ref, cvraw))

    def cache_copy(which, b, to_span, from_span):
        source, landing = cache_pairs[which]
        return pltpu.make_async_remote_copy(
            src_ref=source.at[:, :, columns(to_span)],
            dst_ref=landing.at[from_span],
            send_sem=cache_send.at[which, b - 1],
            recv_sem=cache_recv.at[which, b - 1],
            device_id={"span": to_span},
            device_id_type=MESH,
        )

    own_copies = [
        pltpu.make_async_copy(
            sources[kind].at[:, :, columns(my_group)],
            landings[kind].at[my_slot],
            local_sem.at[kind],
        )
        for kind in range(3)
    ] + [
        pltpu.make_async_copy(
            cache_pairs[which][0].at[:, :, columns(span)],
            cache_pairs[which][1].at[span],
            local_sem.at[3 + which],
        )
        for which in range(2)
    ] + [
        pltpu.make_async_copy(gain_ref.at[:, columns(my_group)], gain, local_sem.at[5])
    ]

    barrier = pltpu.get_barrier_semaphore()

    for k in range(1, n):
        pl.semaphore_signal(barrier, inc=1, device_id=device(ahead(k)), device_id_type=MESH)

    for copy in own_copies:
        copy.start()
    pl.semaphore_wait(barrier, n - 1)

    for b in range(1, n_span):
        for which in range(2):
            cache_copy(which, b, lax.rem(span + b, n_span), span).start()

    flips = {
        1 << b: (1 << b) * (1 - 2 * lax.rem(lax.div(my_group, 1 << b), 2))
        for b in range(n.bit_length() - 1)
    }

    def across(mask):
        group = my_group + sum(flip for bit, flip in flips.items() if mask & bit)
        return lax.div(group, n_span), lax.rem(group, n_span)

    far_masks = [n // 2 + (i % 2) * (n // 4) + i // 2 for i in range(n // 2)]
    near_masks = list(range(n // 4, n // 2)) + list(range(1, n // 4))

    def scatter_all(kind, masks):
        for mask in masks:
            scatter(kind, across(mask)).start()

    alternating = far_masks[:1]
    for pair in zip(near_masks, far_masks[1:]):
        alternating += pair
    scatter_all(KEYS, alternating)
    scatter_all(VALUES, alternating)
    scatter_all(QUERIES, near_masks)

    @pl.when(outer == 0)
    def _():
        scatter_all(QUERIES, far_masks)

    def separate(block, target, row):
        for h in range(heads):
            stage[h] = (
                block[:, :, h * HD : (h + 1) * HD].reshape(members * tokens, HD).astype(jnp.float32)
            )
            for m in range(members):
                target[h * members + m, pl.ds(row, tokens), :] = stage[
                    h, pl.ds(m, tokens, stride=members), :
                ].astype(jnp.bfloat16)

    span_len = n_seq * tokens
    places = lax.broadcasted_iota(jnp.int32, (1, cached), 1)
    live = lax.broadcasted_iota(jnp.int32, (1, span_len), 1)
    for c in range(n_span):
        bias[c : c + 1, 0:cached] = jnp.where(places >= offset_ref[c], 0.0, masked_score)
        for e in range(c + 1):
            first = cached + e * span_len
            bias[c : c + 1, first : first + span_len] = jnp.where(
                live < length_ref[e], 0.0, masked_score
            )
    for copy in own_copies:
        copy.wait()
    levels = lax.broadcasted_iota(jnp.int32, gain.shape, 0)
    for c in range(n_span):
        row_gains[c : c + 1] = jnp.sum(
            jnp.where(levels == step_ref[c], gain[...], 0.0), axis=0, keepdims=True
        )
    for b in range(1, n_span):
        for which in range(2):
            origin = lax.rem(span + n_span - b, n_span)
            cache_copy(which, b, origin, origin).wait_recv()
    for which, target in ((0, kd), (1, vd)):
        for e in range(n_span):

            @pl.loop(0, piece // tokens)
            def _(i, which=which, target=target, e=e):
                row = pl.multiple_of(i * tokens, tokens)
                block = cache_pairs[which][1].at[e, pl.ds(row, tokens)]
                separate(block, target, pl.multiple_of(e * piece + row, tokens))

    def window_row(slot):
        return pl.multiple_of(cached + slot * tokens, tokens)

    for kind, target in ((KEYS, kd), (VALUES, vd)):

        @pl.loop(0, 2 * half)
        def _(i, kind=kind, target=target):
            pair = near_then_far(i)
            arrival(kind, i, pair)

            @pl.loop(0, run)
            def _(r):
                slot = slot_of(member_of(pair, r))
                separate(landings[kind].at[slot], target, window_row(slot))

    @pl.when(outer == 1)
    def _():
        scatter_all(QUERIES, far_masks)

    def turn_lags(t):
        pair = near_then_far(lax.div(t, n_span))
        block_span = lax.rem(t + span, n_span)
        return [lag_from((2 * pair + lax.rem(i + seq, 2), block_span)) for i in range(2)]

    last_pair = n // 2 - n_span

    @pl.loop(0, n // 2)
    def _(t):
        offsets = turn_lags(t)
        block_span = lax.rem(t + span, n_span)

        @pl.when(lax.rem(t, n_span) == 0)
        def _():
            i = lax.div(t, n_span)
            arrival(QUERIES, i, near_then_far(i))

        for i, k in enumerate(offsets):
            separate(qraw.at[slot_of(behind(k))], qd, i * tokens)

        @pl.when((outer == 1) & (t == last_pair))
        def _():
            @pl.loop(half * n_span, last_pair)
            def _(earlier):
                for k in turn_lags(earlier):
                    give_back(k).start()

        for c in range(n_span):

            @pl.when(block_span == c)
            def _(c=c):
                length = cached + (c + 1) * n_seq * tokens

                @pl.loop(0, heads * members)
                def _(g):
                    scores = lax.dot_general(
                        qd[g],
                        kd[g, pl.ds(0, length), :],
                        (((1,), (1,)), ((), ())),
                        preferred_element_type=jnp.float32,
                    )
                    scores = scores * scale + bias[c : c + 1, pl.ds(0, length)]
                    largest = jnp.max(scores, axis=1, keepdims=True)
                    weights = jnp.exp(scores - largest)
                    total = jnp.sum(weights, axis=1, keepdims=True)
                    od[g] = (
                        jnp.dot(
                            weights.astype(jnp.bfloat16),
                            vd[g, pl.ds(0, length), :],
                            preferred_element_type=jnp.float32,
                        )
                        / total
                    )

                for i, k in enumerate(offsets):
                    for h in range(heads):
                        row_gain = row_gains[c : c + 1, h * HD : (h + 1) * HD]
                        for m in range(members):
                            stage[h, pl.ds(m, tokens, stride=members), :] = (
                                od[h * members + m, i * tokens : (i + 1) * tokens, :] * row_gain
                            )
                        oraw[k, :, :, h * HD : (h + 1) * HD] = (
                            stage[h].astype(jnp.bfloat16).reshape(tokens, members, HD)
                        )

        held_back = (outer == 1) & (t >= half * n_span) & (t < last_pair)
        for k in offsets:

            @pl.when((k > 0) & jnp.logical_not(held_back))
            def _(k=k):
                give_back(k).start()

    last = pltpu.make_async_copy(
        oraw.at[0], out_ref.at[:, :, columns(my_group)], local_sem.at[6]
    )
    last.start()

    for kind in range(4):
        take(n - 1, send_sem.at[kind])
    take(n - 1, back_sem)

    for b in range(1, n_span):
        for which in range(2):
            cache_copy(which, b, lax.rem(span + b, n_span), span).wait_send()
    last.wait()


def hand_over(pieces, source, target, sem):
    rows = source.shape[0] // pieces
    outward = [
        pltpu.make_async_copy(
            source.at[pl.ds(i * rows, rows)], target.at[pl.ds(i * rows, rows)], sem.at[i]
        )
        for i in range(pieces)
    ]
    for copy in outward:
        copy.start()
    for copy in outward:
        copy.wait()


def per_device(
    queries,
    keys,
    values,
    cache_keys,
    cache_values,
    span_lengths,
    cache_offsets,
    step_index,
    step_gain,
):
    n_seq, n_span = lax.axis_size("seq"), lax.axis_size("span")
    n = n_seq * n_span
    tokens, members, features = queries.shape
    width = features // n
    groups = members * width // HD
    piece = cache_keys.shape[0]
    cached, span_len = n_span * piece, n_seq * tokens
    full = cached + n_span * span_len

    anywhere = pl.BlockSpec(memory_space=pl.ANY)
    scalars = pl.BlockSpec(memory_space=pltpu.SMEM)
    block = (n, tokens, members, width)
    attended = pl.pallas_call(
        functools.partial(kernel, n_seq, n_span),
        out_shape=pltpu.VMEM(queries.shape, jnp.bfloat16),
        in_specs=[anywhere] * 5 + [scalars] * 3 + [anywhere],
        out_specs=pl.BlockSpec(memory_space=pltpu.VMEM),
        scratch_shapes=[pltpu.VMEM(block, jnp.bfloat16)] * 4
        + [pltpu.VMEM((n_span, piece, members, width), jnp.bfloat16)] * 2
        + [pltpu.VMEM((groups, full, HD), jnp.bfloat16)] * 2
        + [
            pltpu.VMEM((groups, 2 * tokens, HD), jnp.bfloat16),
            pltpu.VMEM((groups, 2 * tokens, HD), jnp.float32),
            pltpu.VMEM((width // HD, members * tokens, HD), jnp.float32),
            pltpu.VMEM((n_span, full), jnp.float32),
            pltpu.VMEM((step_gain.shape[0], width), jnp.float32),
            pltpu.VMEM((n_span, width), jnp.float32),
            pltpu.SemaphoreType.DMA((4,)),
            pltpu.SemaphoreType.DMA((3, n_seq // 2)),
            pltpu.SemaphoreType.DMA,
            pltpu.SemaphoreType.DMA((2, n_span - 1)),
            pltpu.SemaphoreType.DMA((2, n_span - 1)),
            pltpu.SemaphoreType.DMA((7,)),
        ],
        compiler_params=pltpu.CompilerParams(
            collective_id=0, has_side_effects=True, vmem_limit_bytes=60 * 2**20
        ),
    )(
        queries,
        keys,
        values,
        cache_keys,
        cache_values,
        span_lengths,
        cache_offsets,
        step_index,
        step_gain,
    )
    pieces = 4
    return pl.pallas_call(
        functools.partial(hand_over, pieces),
        out_shape=jax.ShapeDtypeStruct(queries.shape, jnp.bfloat16),
        in_specs=[pl.BlockSpec(memory_space=pltpu.VMEM)],
        out_specs=anywhere,
        scratch_shapes=[pltpu.SemaphoreType.DMA((pieces,))],
        compiler_params=pltpu.CompilerParams(vmem_limit_bytes=16 * 2**20),
    )(attended)


def solution(mesh):
    placed = (
        P(("rep", "span", "seq"), None, None),
        P(("rep", "span", "seq"), None, None),
        P(("rep", "span", "seq"), None, None),
        P(("rep", "span"), None, "seq"),
        P(("rep", "span"), None, "seq"),
        P("rep"),
        P("rep"),
        P("rep"),
        P(),
    )
    return jax.shard_map(
        per_device,
        mesh=mesh,
        in_specs=placed,
        out_specs=P(("rep", "span", "seq"), None, None),
        check_vma=False,
    )
```

```python
import functools

import jax
import jax.numpy as jnp
from jax import lax
from jax.experimental import pallas as pl
from jax.experimental.pallas import tpu as pltpu
from jax.sharding import PartitionSpec as P

HD = 128
MESH = pl.DeviceIdType.MESH
masked_score = -1e30
KEYS, VALUES, QUERIES, OUTS = range(4)


def kernel(
    n_seq,
    n_span,
    q_ref,
    k_ref,
    v_ref,
    ck_ref,
    cv_ref,
    length_ref,
    offset_ref,
    step_ref,
    gain_ref,
    out_ref,
    kraw,
    vraw,
    qraw,
    oraw,
    ckraw,
    cvraw,
    kd,
    vd,
    qd,
    od,
    stage,
    bias,
    gain,
    row_gains,
    send_sem,
    recv_sem,
    back_sem,
    cache_send,
    cache_recv,
    local_sem,
    late_sem,
):
    n = n_seq * n_span
    seq, span = lax.axis_index("seq"), lax.axis_index("span")
    tokens, members, width = kraw.shape[1:]
    heads = width // HD
    piece = ckraw.shape[1]
    cached = n_span * piece
    scale = HD ** (-0.5)
    my_group = seq * n_span + span
    my_slot = span * n_seq + seq

    def ahead(k):
        return (
            lax.rem(seq + lax.div(k, n_span), n_seq),
            lax.rem(span + lax.rem(k, n_span), n_span),
        )

    def behind(k):
        return (
            lax.rem(seq + n_seq - lax.div(k, n_span), n_seq),
            lax.rem(span + n_span - lax.rem(k, n_span), n_span),
        )

    half = n_seq // 4
    run = 2 * n_span
    my_pair = lax.div(seq, 2)
    upper = lax.div(my_pair, half)
    lower = 1 - upper
    depth = my_pair - upper * half
    outer = lower * (1 - lax.div(depth, half - half // 2)) + upper * lax.div(depth, half // 2)

    def near_pair(i):
        return upper * half + lax.rem(depth + i, half)

    def far_pair(i):
        return lower * (2 * half - 1 - i) + upper * i

    def near_then_far(i):
        far = lax.div(i, half)
        return (1 - far) * near_pair(i) + far * far_pair(i - half)

    def member_of(pair, r):
        return (2 * pair + lax.div(r, n_span), lax.rem(r, n_span))

    def lag_from(place):
        return lax.rem(seq - place[0] + n_seq, n_seq) * n_span + lax.rem(
            span - place[1] + n_span, n_span
        )

    def columns(group):
        return pl.ds(pl.multiple_of(group * width, HD), width)

    def group_of(place):
        return place[0] * n_span + place[1]

    def slot_of(place):
        return place[1] * n_seq + place[0]

    def device(place):
        return {"seq": place[0], "span": place[1]}

    sources = (k_ref, v_ref, q_ref)
    landings = (kraw, vraw, qraw)

    def scatter(kind, to):
        return pltpu.make_async_remote_copy(
            src_ref=sources[kind].at[:, :, columns(group_of(to))],
            dst_ref=landings[kind].at[my_slot],
            send_sem=send_sem.at[kind],
            recv_sem=recv_sem.at[kind, my_pair],
            device_id=device(to),
            device_id_type=MESH,
        )

    def take(blocks, sem):
        many = kraw.at[pl.ds(0, blocks)]
        pltpu.make_async_copy(many, many, sem).wait()

    def arrival(kind, i, pair):
        @pl.when(i == 0)
        def _():
            take(run - 1, recv_sem.at[kind, pair])

        @pl.when(i > 0)
        def _():
            take(run, recv_sem.at[kind, pair])

    def give_back(k):
        to = behind(k)
        return pltpu.make_async_remote_copy(
            src_ref=oraw.at[k],
            dst_ref=out_ref.at[:, :, columns(my_group)],
            send_sem=send_sem.at[OUTS],
            recv_sem=back_sem,
            device_id=device(to),
            device_id_type=MESH,
        )

    cache_pairs = ((ck_ref, ckraw), (cv_ref, cvraw))

    def cache_copy(which, b, to_span, from_span):
        source, landing = cache_pairs[which]
        return pltpu.make_async_remote_copy(
            src_ref=source.at[:, :, columns(to_span)],
            dst_ref=landing.at[from_span],
            send_sem=cache_send.at[which, b - 1],
            recv_sem=cache_recv.at[which, b - 1],
            device_id={"span": to_span},
            device_id_type=MESH,
        )

    own_copies = [
        pltpu.make_async_copy(
            sources[kind].at[:, :, columns(my_group)],
            landings[kind].at[my_slot],
            local_sem.at[kind],
        )
        for kind in range(3)
    ] + [
        pltpu.make_async_copy(
            cache_pairs[which][0].at[:, :, columns(span)],
            cache_pairs[which][1].at[span],
            local_sem.at[3 + which],
        )
        for which in range(2)
    ] + [
        pltpu.make_async_copy(gain_ref.at[:, columns(my_group)], gain, local_sem.at[5])
    ]

    barrier = pltpu.get_barrier_semaphore()

    flips = {
        1 << b: (1 << b) * (1 - 2 * lax.rem(lax.div(my_group, 1 << b), 2))
        for b in range(n.bit_length() - 1)
    }

    def across(mask):
        group = my_group + sum(flip for bit, flip in flips.items() if mask & bit)
        return lax.div(group, n_span), lax.rem(group, n_span)

    def greet(masks, sem):
        for mask in masks:
            pl.semaphore_signal(
                sem, inc=1, device_id=device(across(mask)), device_id_type=MESH
            )

    alike = list(range(3 * n // 4, n)) + list(range(1, n // 4))
    unlike = list(range(n // 4, 3 * n // 4))
    early = alike[:1]

    @pl.when(outer == 0)
    def _():
        greet(unlike, barrier)

    greet(alike, barrier)
    for copy in own_copies:
        copy.start()

    @pl.when(outer == 0)
    def _():
        pl.semaphore_wait(barrier, len(alike))
        for mask in early:
            scatter(KEYS, across(mask)).start()
        pl.semaphore_wait(late_sem, len(unlike))

    @pl.when(outer == 1)
    def _():
        pl.semaphore_wait(barrier, n - 1)
        greet(unlike, late_sem)
        for mask in early:
            scatter(KEYS, across(mask)).start()

    for b in range(1, n_span):
        for which in range(2):
            cache_copy(which, b, lax.rem(span + b, n_span), span).start()

    far_masks = [n // 2 + (i % 2) * (n // 4) + i // 2 for i in range(n // 2)]
    near_masks = list(range(n // 4, n // 2)) + list(range(1, n // 4))

    def scatter_all(kind, masks):
        for mask in masks:
            scatter(kind, across(mask)).start()

    alternating = far_masks[:1]
    for pair in zip(near_masks, far_masks[1:]):
        alternating += pair
    scatter_all(KEYS, [mask for mask in alternating if mask not in early])
    scatter_all(VALUES, alternating)
    scatter_all(QUERIES, near_masks)

    @pl.when(outer == 0)
    def _():
        scatter_all(QUERIES, far_masks)

    def separate(block, target, row):
        for h in range(heads):
            stage[h] = (
                block[:, :, h * HD : (h + 1) * HD].reshape(members * tokens, HD).astype(jnp.float32)
            )
            for m in range(members):
                target[h * members + m, pl.ds(row, tokens), :] = stage[
                    h, pl.ds(m, tokens, stride=members), :
                ].astype(jnp.bfloat16)

    span_len = n_seq * tokens
    places = lax.broadcasted_iota(jnp.int32, (1, cached), 1)
    live = lax.broadcasted_iota(jnp.int32, (1, span_len), 1)
    for c in range(n_span):
        bias[c : c + 1, 0:cached] = jnp.where(places >= offset_ref[c], 0.0, masked_score)
        for e in range(c + 1):
            first = cached + e * span_len
            bias[c : c + 1, first : first + span_len] = jnp.where(
                live < length_ref[e], 0.0, masked_score
            )
    for copy in own_copies:
        copy.wait()
    levels = lax.broadcasted_iota(jnp.int32, gain.shape, 0)
    for c in range(n_span):
        row_gains[c : c + 1] = jnp.sum(
            jnp.where(levels == step_ref[c], gain[...], 0.0), axis=0, keepdims=True
        )
    for b in range(1, n_span):
        for which in range(2):
            origin = lax.rem(span + n_span - b, n_span)
            cache_copy(which, b, origin, origin).wait_recv()
    for which, target in ((0, kd), (1, vd)):
        for e in range(n_span):

            @pl.loop(0, piece // tokens)
            def _(i, which=which, target=target, e=e):
                row = pl.multiple_of(i * tokens, tokens)
                block = cache_pairs[which][1].at[e, pl.ds(row, tokens)]
                separate(block, target, pl.multiple_of(e * piece + row, tokens))

    def window_row(slot):
        return pl.multiple_of(cached + slot * tokens, tokens)

    for kind, target in ((KEYS, kd), (VALUES, vd)):

        @pl.loop(0, 2 * half)
        def _(i, kind=kind, target=target):
            pair = near_then_far(i)
            arrival(kind, i, pair)

            @pl.loop(0, run)
            def _(r):
                slot = slot_of(member_of(pair, r))
                separate(landings[kind].at[slot], target, window_row(slot))

    @pl.when(outer == 1)
    def _():
        scatter_all(QUERIES, far_masks)

    def turn_lags(t):
        pair = near_then_far(lax.div(t, n_span))
        block_span = lax.rem(t, n_span)
        return [lag_from((2 * pair + i, block_span)) for i in range(2)]

    last_pair = n // 2 - n_span

    @pl.loop(0, n // 2)
    def _(t):
        offsets = turn_lags(t)
        block_span = lax.rem(t, n_span)

        @pl.when(lax.rem(t, n_span) == 0)
        def _():
            i = lax.div(t, n_span)
            arrival(QUERIES, i, near_then_far(i))

        for i, k in enumerate(offsets):
            separate(qraw.at[slot_of(behind(k))], qd, i * tokens)

        @pl.when((outer == 1) & (t == last_pair))
        def _():
            @pl.loop(half * n_span, last_pair)
            def _(earlier):
                for k in turn_lags(earlier):
                    give_back(k).start()

        for c in range(n_span):

            @pl.when(block_span == c)
            def _(c=c):
                length = cached + (c + 1) * n_seq * tokens

                @pl.loop(0, heads * members)
                def _(g):
                    scores = lax.dot_general(
                        qd[g],
                        kd[g, pl.ds(0, length), :],
                        (((1,), (1,)), ((), ())),
                        preferred_element_type=jnp.float32,
                    )
                    scores = scores * scale + bias[c : c + 1, pl.ds(0, length)]
                    largest = jnp.max(scores, axis=1, keepdims=True)
                    weights = jnp.exp(scores - largest)
                    total = jnp.sum(weights, axis=1, keepdims=True)
                    od[g] = (
                        jnp.dot(
                            weights.astype(jnp.bfloat16),
                            vd[g, pl.ds(0, length), :],
                            preferred_element_type=jnp.float32,
                        )
                        / total
                    )

                for i, k in enumerate(offsets):
                    for h in range(heads):
                        row_gain = row_gains[c : c + 1, h * HD : (h + 1) * HD]
                        for m in range(members):
                            stage[h, pl.ds(m, tokens, stride=members), :] = (
                                od[h * members + m, i * tokens : (i + 1) * tokens, :] * row_gain
                            )
                        oraw[k, :, :, h * HD : (h + 1) * HD] = (
                            stage[h].astype(jnp.bfloat16).reshape(tokens, members, HD)
                        )

        held_back = (outer == 1) & (t >= half * n_span) & (t < last_pair)
        for k in offsets:

            @pl.when((k > 0) & jnp.logical_not(held_back))
            def _(k=k):
                give_back(k).start()

    last = pltpu.make_async_copy(
        oraw.at[0], out_ref.at[:, :, columns(my_group)], local_sem.at[6]
    )
    last.start()

    for kind in range(4):
        take(n - 1, send_sem.at[kind])
    take(n - 1, back_sem)

    for b in range(1, n_span):
        for which in range(2):
            cache_copy(which, b, lax.rem(span + b, n_span), span).wait_send()
    last.wait()


def hand_over(pieces, source, target, sem):
    rows = source.shape[0] // pieces
    outward = [
        pltpu.make_async_copy(
            source.at[pl.ds(i * rows, rows)], target.at[pl.ds(i * rows, rows)], sem.at[i]
        )
        for i in range(pieces)
    ]
    for copy in outward:
        copy.start()
    for copy in outward:
        copy.wait()


def per_device(
    queries,
    keys,
    values,
    cache_keys,
    cache_values,
    span_lengths,
    cache_offsets,
    step_index,
    step_gain,
):
    n_seq, n_span = lax.axis_size("seq"), lax.axis_size("span")
    n = n_seq * n_span
    tokens, members, features = queries.shape
    width = features // n
    groups = members * width // HD
    piece = cache_keys.shape[0]
    cached, span_len = n_span * piece, n_seq * tokens
    full = cached + n_span * span_len

    anywhere = pl.BlockSpec(memory_space=pl.ANY)
    scalars = pl.BlockSpec(memory_space=pltpu.SMEM)
    block = (n, tokens, members, width)
    attended = pl.pallas_call(
        functools.partial(kernel, n_seq, n_span),
        out_shape=pltpu.VMEM(queries.shape, jnp.bfloat16),
        in_specs=[anywhere] * 5 + [scalars] * 3 + [anywhere],
        out_specs=pl.BlockSpec(memory_space=pltpu.VMEM),
        scratch_shapes=[pltpu.VMEM(block, jnp.bfloat16)] * 4
        + [pltpu.VMEM((n_span, piece, members, width), jnp.bfloat16)] * 2
        + [pltpu.VMEM((groups, full, HD), jnp.bfloat16)] * 2
        + [
            pltpu.VMEM((groups, 2 * tokens, HD), jnp.bfloat16),
            pltpu.VMEM((groups, 2 * tokens, HD), jnp.float32),
            pltpu.VMEM((width // HD, members * tokens, HD), jnp.float32),
            pltpu.VMEM((n_span, full), jnp.float32),
            pltpu.VMEM((step_gain.shape[0], width), jnp.float32),
            pltpu.VMEM((n_span, width), jnp.float32),
            pltpu.SemaphoreType.DMA((4,)),
            pltpu.SemaphoreType.DMA((3, n_seq // 2)),
            pltpu.SemaphoreType.DMA,
            pltpu.SemaphoreType.DMA((2, n_span - 1)),
            pltpu.SemaphoreType.DMA((2, n_span - 1)),
            pltpu.SemaphoreType.DMA((7,)),
            pltpu.SemaphoreType.REGULAR,
        ],
        compiler_params=pltpu.CompilerParams(
            collective_id=0, has_side_effects=True, vmem_limit_bytes=60 * 2**20
        ),
    )(
        queries,
        keys,
        values,
        cache_keys,
        cache_values,
        span_lengths,
        cache_offsets,
        step_index,
        step_gain,
    )
    pieces = 4
    return pl.pallas_call(
        functools.partial(hand_over, pieces),
        out_shape=jax.ShapeDtypeStruct(queries.shape, jnp.bfloat16),
        in_specs=[pl.BlockSpec(memory_space=pltpu.VMEM)],
        out_specs=anywhere,
        scratch_shapes=[pltpu.SemaphoreType.DMA((pieces,))],
        compiler_params=pltpu.CompilerParams(vmem_limit_bytes=16 * 2**20),
    )(attended)


def solution(mesh):
    placed = (
        P(("rep", "span", "seq"), None, None),
        P(("rep", "span", "seq"), None, None),
        P(("rep", "span", "seq"), None, None),
        P(("rep", "span"), None, "seq"),
        P(("rep", "span"), None, "seq"),
        P("rep"),
        P("rep"),
        P("rep"),
        P(),
    )
    return jax.shard_map(
        per_device,
        mesh=mesh,
        in_specs=placed,
        out_specs=P(("rep", "span", "seq"), None, None),
        check_vma=False,
    )
```
